128 devices in a mesh: grp: 32 (over x, z, core), tp: 4 (over y).
Axes of the slice: x: 4, y: 4, z: 4, core: 2. Of those that a mesh axis runs over, the one named last changes fastest.
Arguments:
- q_nope: bfloat16 [2048, 16384], P('grp', 'tp'), may hold values from -6 to 6
- q_rope: bfloat16 [2048, 8192], P('grp', 'tp'), may hold values from -500 to 500
- w_uk: bfloat16 [128, 128, 512], P('tp'), may hold values from -0.5 to 0.5
- w_uv: bfloat16 [128, 512, 128], P('tp'), may hold values from -1 to 1
- prefix_latent: bfloat16 [64, 2048, 512], P('grp'), may hold values from -5 to 5
- prefix_rope: bfloat16 [64, 64, 2048], P('grp'), may hold values from -8 to 8
- suffix_latent: bfloat16 [2048, 256, 512], P(('grp', 'tp')), may hold values from -5 to 5
- suffix_rope: bfloat16 [2048, 64, 256], P(('grp', 'tp')), may hold values from -4 to 4
- suffix_len: int32 [32, 64], P('grp'), may hold values from 1 to 256, 8192 in all within a row
- request_prefix: int32 [2048], P('grp'), may hold values from 0 to 63, as said below
- prefix_slot: int32 [64], replicated, may hold values from 0 to 63, as said below
Outputs:
- attended: bfloat16 [2048, 16384], P('grp', 'tp')
The draws below stay inside these ranges and needn't reach their ends.
Inputs may be any that keep to these rules, and one draw needn't show every extreme that they name: `request_prefix`: of the requests of one group, at most 2 name the same prefix; in every draw one prefix is named by exactly 2 requests of every group. `prefix_slot`: A permutation: each cache row holds exactly one prefix. `suffix_len`: the lengths of one group sum to 8192, and one of them is 256.
All inputs are finite; a program needn't handle non-finite values.
Results may differ from the reference program's by a relative error of at most 0.018.
Values may be sent and summed in bfloat16 or wider, within the bound.
A program may use at most 128 MiB of HBM per device.

```python
import math
import jax
import jax.numpy as jnp
import numpy as np
from jax import lax

HEADS = 128
LATENT = 512
ROPE_DIM = 64
NOPE_DIM = 128
VALUE_DIM = 128
REQ_DEV = 64
PLEN = 2048
SLEN = 256
GROUPS = 32
PREFIXES = 64
CAPP = 2
REQUESTS = 2048


def route_draw(key):
    base_key = jax.random.fold_in(key, 101)
    hot_slot = jax.random.randint(jax.random.fold_in(base_key, 1), (), 0, PREFIXES)
    scores = jax.random.randint(jax.random.fold_in(base_key, 2), (GROUPS, PREFIXES * CAPP), 0, 1073741824)
    position = jnp.arange(PREFIXES * CAPP, dtype=jnp.int32)
    scores = jnp.where((position // CAPP)[None, :] == hot_slot, -1, scores)
    ranked = jnp.argsort(scores, axis=1, stable=True)[:, :REQ_DEV]
    shuffle_keys = jax.random.randint(jax.random.fold_in(base_key, 3), (GROUPS, REQ_DEV), 0, 1073741824)
    shuffle = jnp.argsort(shuffle_keys, axis=1, stable=True)
    chosen = jnp.take_along_axis(ranked, shuffle, axis=1)
    slot_ids = (chosen // CAPP).reshape(-1).astype(jnp.int32)
    permuted = jax.random.permutation(jax.random.fold_in(base_key, 4), PREFIXES).astype(jnp.int32)
    inverse = jnp.argsort(permuted).astype(jnp.int32)
    return (inverse[slot_ids], permuted)


def rope_table(key):
    drawn = jnp.clip(jax.random.normal(jax.random.fold_in(key, 202), (PREFIXES, ROPE_DIM, PLEN), jnp.float32), -4.0, 4.0)
    return drawn


def draw_request_prefix(key, part):
    return route_draw(key)[0]


def draw_prefix_slot(key, part):
    return route_draw(key)[1]


def draw_prefix_rope(key, part):
    return rope_table(key).astype(jnp.bfloat16)


def draw_q_rope(key, part):
    drawn = jnp.clip(jax.random.normal(jax.random.fold_in(key, 303), (REQUESTS, HEADS * ROPE_DIM), jnp.float32), -4.0, 4.0)
    return drawn.astype(jnp.bfloat16)


def shard_levels(key, dims, cuts, low, high):
    factor_of = 1.0
    for dim, parts in cuts:
        heights = jax.random.uniform(jax.random.fold_in(jax.random.fold_in(key, 6), dim), (parts,), jnp.float32, low / len(cuts), high / len(cuts))
        factor_of = factor_of * jnp.repeat(jnp.exp(heights), dims[dim] // parts).reshape((-1,) + (1,) * (len(dims) - 1 - dim))
    return factor_of


def length_profile(number_of, total, limit, skew):
    weights = [(1 << 20) // math.isqrt(standing ** skew) + 1 for standing in range(2, number_of + 1)]
    surplus, counts = total - limit - (number_of - 1), [1] * (number_of - 1)
    while surplus > 0:
        candidates = [i for i in range(number_of - 1) if counts[i] < limit]
        whole, budget = sum([weights[i] for i in candidates]), surplus
        for i in candidates:
            addition = min(limit - counts[i], max(1, budget * weights[i] // whole), surplus)
            counts[i] = counts[i] + addition
            surplus = surplus - addition
    return np.array([limit] + counts)


def uneven(stream_key, amount, total, limit, slope):
    if amount == 2:
        one = jax.random.randint(stream_key, (), max(1, total - limit), min(limit, total - 1) + 1)
        return jnp.stack([one, total - one])
    sizes = jnp.asarray(length_profile(amount, total, limit, slope), jnp.int32)
    couples = (amount - 1) // 2
    donor, receiver = sizes[1:1 + 2 * couples:2], sizes[2:2 + 2 * couples:2]
    slack = jnp.minimum(donor - 1, limit - receiver)
    shifted = jax.random.randint(jax.random.fold_in(stream_key, 1), (couples,), 0, 1 << 20) % (slack + 1)
    sizes = sizes.at[1:1 + 2 * couples:2].set(donor - shifted).at[2:2 + 2 * couples:2].set(receiver + shifted)
    return sizes[jax.random.permutation(jax.random.fold_in(stream_key, 2), amount)]


def normal_values(key, extent, spread, bound, pieces=(), kind=jnp.bfloat16):
    values = jax.random.normal(key, extent, jnp.float32) * spread
    if len(pieces) > 0:
        values = shard_levels(key, extent, pieces, -0.22, 0.18) * values
    return jnp.clip(values, min=-bound, max=bound).astype(kind)


def setup_inputs(seed: int = 0) -> dict:
    seeds = jax.random.split(jax.random.key(seed), 12)
    q_nope = normal_values(seeds[0], (REQUESTS, HEADS * NOPE_DIM), 1.25, 6.0, ((0, 32), (1, 4)))
    q_rope = draw_q_rope(jax.random.fold_in(seeds[11], 71), 0)
    w_uk = normal_values(seeds[2], (HEADS, NOPE_DIM, LATENT), NOPE_DIM ** -0.5, 0.5, ((0, 4),))
    w_uv = normal_values(seeds[3], (HEADS, LATENT, VALUE_DIM), (LATENT // 16) ** -0.5, 1.0, ((0, 4),))
    prefix_latent = normal_values(seeds[4], (PREFIXES, PLEN, LATENT), 1.0, 5.0, ((0, 32),))
    prefix_rope = draw_prefix_rope(jax.random.fold_in(seeds[11], 71), 0)
    suffix_latent = normal_values(seeds[6], (REQUESTS, SLEN, LATENT), 1.0, 5.0, ((0, 128),))
    suffix_rope = normal_values(seeds[7], (REQUESTS, ROPE_DIM, SLEN), 1.0, 4.0, ((0, 128),))
    suffix_len = jax.vmap(lambda own: uneven(own, REQ_DEV, REQ_DEV * SLEN // 2, SLEN, 2))(jax.random.split(seeds[8], GROUPS)).reshape((GROUPS, REQ_DEV)).astype(jnp.int32)
    request_prefix = draw_request_prefix(jax.random.fold_in(seeds[11], 71), 0)
    prefix_slot = draw_prefix_slot(jax.random.fold_in(seeds[11], 71), 0)
    return {"q_nope": q_nope, "q_rope": q_rope, "w_uk": w_uk, "w_uv": w_uv, "prefix_latent": prefix_latent, "prefix_rope": prefix_rope, "suffix_latent": suffix_latent, "suffix_rope": suffix_rope, "suffix_len": suffix_len, "request_prefix": request_prefix, "prefix_slot": prefix_slot}


def partial_attention(latent_q, rope_q, latent_rows, rope_cols, live_mask, score_scale):
    scores = jnp.dot(latent_q, latent_rows.T, preferred_element_type=jnp.float32)
    scores = (scores + jnp.dot(rope_q, rope_cols, preferred_element_type=jnp.float32)) * score_scale
    scores = jnp.where(live_mask[None, :], scores, jnp.float32(-1e+30))
    highest = lax.optimization_barrier(jnp.max(scores, axis=1, keepdims=True))
    exponent = jnp.where(live_mask[None, :], jnp.exp(scores - highest), jnp.float32(0.0))
    summed = lax.optimization_barrier(jnp.sum(exponent, axis=1))
    weights = exponent.astype(jnp.bfloat16)
    latent_out = (jnp.dot(weights, latent_rows, preferred_element_type=jnp.float32) / summed[:, None]).astype(jnp.bfloat16)
    return (latent_out, highest[:, 0], summed)

def reference(q_nope, q_rope, w_uk, w_uv, prefix_latent, prefix_rope, suffix_latent, suffix_rope, suffix_len, request_prefix, prefix_slot):
    score_scale = 1.0 / math.sqrt(NOPE_DIM + ROPE_DIM)
    slot_ids = prefix_slot[request_prefix].astype(jnp.int32)
    lengths = suffix_len.reshape(-1).astype(jnp.int32)
    nope_heads = q_nope.reshape(REQUESTS, HEADS, NOPE_DIM).astype(jnp.float32)
    q_latent = jnp.einsum('rhd,hdc->rhc', nope_heads, w_uk.astype(jnp.float32)).astype(jnp.bfloat16)
    rope_heads = q_rope.reshape(REQUESTS, HEADS, ROPE_DIM)
    w_uv_wide = w_uv.astype(jnp.float32)
    positions = jnp.arange(SLEN, dtype=jnp.int32)
    prefix_live = jnp.ones((PLEN,), dtype=bool)

    def one_request(request_items):
        latent_q, rope_q, slot_id, suffix_rows, suffix_cols, length = request_items
        latent_rows = lax.dynamic_index_in_dim(prefix_latent, slot_id, 0, keepdims=False)
        rope_cols = lax.dynamic_index_in_dim(prefix_rope, slot_id, 0, keepdims=False)
        prefix_out, prefix_max, prefix_total = partial_attention(latent_q, rope_q, latent_rows, rope_cols, prefix_live, score_scale)
        prefix_values = jnp.einsum('hc,hcv->hv', prefix_out.astype(jnp.float32), w_uv_wide).astype(jnp.bfloat16)
        suffix_live = positions < length
        suffix_out, suffix_max, suffix_total = partial_attention(latent_q, rope_q, suffix_rows, suffix_cols, suffix_live, score_scale)
        suffix_values = jnp.einsum('hc,hcv->hv', suffix_out.astype(jnp.float32), w_uv_wide).astype(jnp.bfloat16)
        overall = jnp.maximum(prefix_max, suffix_max)
        prefix_share = prefix_total * jnp.exp(prefix_max - overall)
        suffix_share = suffix_total * jnp.exp(suffix_max - overall)
        mixed = prefix_share[:, None] * prefix_values.astype(jnp.float32) + suffix_share[:, None] * suffix_values.astype(jnp.float32)
        mixed = mixed / (prefix_share + suffix_share)[:, None]
        return mixed.astype(jnp.bfloat16).reshape(-1)
    return lax.map(one_request, (q_latent, rope_heads, slot_ids, suffix_latent, suffix_rope, lengths))
```

```python
import math

import jax
import jax.numpy as jnp
from jax import lax
from jax.experimental import pallas as pl
from jax.experimental.pallas import tpu as pltpu
from jax.sharding import PartitionSpec as P

MESH = pl.DeviceIdType.MESH
BF, F32, I32 = jnp.bfloat16, jnp.float32, jnp.int32
LATENT, ROPE, NOPE, VALUE = 512, 64, 128, 128
PLEN, SLEN = 2048, 256
HEADS, REQS, OWN, GROUPS, TP = 32, 64, 16, 32, 4
SCALE = 1.0 / math.sqrt(NOPE + ROPE)
SCALE2 = SCALE * math.log2(math.e)
STATS = 128


def dot(a, b):
    return jnp.dot(a, b, preferred_element_type=F32)


def iota(shape, dim):
    return lax.broadcasted_iota(I32, shape, dim)


def onehot(mask):
    return jnp.where(mask, 1.0, 0.0).astype(BF)


def kernel(
    qn, qr, wuk, wuv, plat, prope, slat, srope, rp, ps, slen, out,
    qn_v, qr_v, wuk_v, wuv_v, pl_v, kt_v, sl_v, skr_v,
    sel_v, selt_v, perm_v, slots_v, slotst_v,
    xlat_v, yslat, yrlat, ysrope, yrrope, o_v, ybs, ybr, stat_v, ybs_st, ybr_st,
    xs, xr, qperm, vb, pst, bs0, br0, bs1, br1,
    qb0, qb1, s0, s1, pb0, pb1, out_v,
    lsem, osem, yss, yrs, yrss, yrrs, bss, brs, bsts, brts, xss, xrs, zss, zrs,
):
    g, t = lax.axis_index("grp"), lax.axis_index("tp")
    bar = pltpu.get_barrier_semaphore()
    for k in range(1, TP):
        pl.semaphore_signal(bar, inc=1, device_id=(g, lax.rem(t + k, TP)), device_id_type=MESH)

    def greet(k, c):
        pl.semaphore_signal(bar, inc=1, device_id=(lax.rem(g + k, GROUPS), t), device_id_type=MESH)
        return c

    lax.fori_loop(1, GROUPS, greet, 0)

    def rel(k):
        return pl.multiple_of(lax.rem(t + k, TP) * OWN, OWN)

    for k in range(TP):
        rows = pl.ds(k * OWN, OWN)
        pltpu.make_async_copy(qn.at[pl.ds(rel(k), OWN)], qn_v.at[rows], lsem.at[0]).start()
        pltpu.make_async_copy(qr.at[pl.ds(rel(k), OWN)], qr_v.at[rows], lsem.at[1]).start()
    loads = [(wuk, wuk_v)]
    for p in range(2):
        loads.append((plat.at[p], pl_v.at[p]))
        for b in range(2):
            loads.append((prope.at[p], kt_v.at[p, pl.ds(LATENT + b * ROPE, ROPE)]))
    loads.append((slat, sl_v))
    for b in range(2):
        loads.append((srope, skr_v.at[:, pl.ds(b * ROPE, ROPE)]))
    loads.append((wuv, wuv_v))
    copies = [pltpu.make_async_copy(a, b, lsem.at[2 + i]) for i, (a, b) in enumerate(loads)]
    for c in copies:
        c.start()
    ld_wuk, ld_p, ld_s, ld_wuv = copies[0], (copies[1:4], copies[4:7]), copies[7:10], copies[10]

    shift = lax.rem(128 - OWN * t, 128)
    named = pltpu.roll(rp[...].astype(F32), shift, 1)[0:1]
    sq = (128, 128)
    first = iota(sq, 0)
    slot_of = jnp.broadcast_to(ps[...].astype(F32)[0:1], sq).T
    hit = jnp.broadcast_to(named, sq) == first.astype(F32)
    slot = jnp.sum(jnp.where(hit, slot_of, 0.0), axis=0, keepdims=True)
    slot_b = jnp.broadcast_to(slot, sq)
    before = first < (iota(sq, 1) & 63)
    rank = jnp.sum(
        jnp.where(before & (slot_b.T == slot_b), 1.0, 0.0), axis=0, keepdims=True
    )
    buf = jnp.broadcast_to(2.0 * slot + rank, sq)
    buf_r = buf.astype(I32)
    buf_c = buf.T.astype(I32)
    for b in range(4):
        i, j = iota(sq, 0) + b * 128, iota(sq, 1)
        key, col = (i >> 4) * 4 + (i & 3), (i >> 2) & 3
        for e in range(2):
            sel_v[b * 128 : b * 128 + 128, e * 128 : e * 128 + 128] = onehot(
                (key == buf_r) & (col == ((j + e * 128) >> 6))
            )
        i, j = iota(sq, 0), iota(sq, 1) + b * 128
        key, col = (j >> 4) * 4 + (j & 3), (j >> 2) & 3
        for e in range(2):
            selt_v[e * 128 : e * 128 + 128, b * 128 : b * 128 + 128] = onehot(
                (key == buf_c) & (col == ((i + e * 128) >> 6))
            )
    i, j = iota((256, 256), 0), iota((256, 256), 1)
    perm_v[...] = onehot(j == (i & 15) * 16 + (i >> 4))
    for b in range(4):
        i, j = iota((128, 512), 0) + b * 128, iota((128, 512), 1)
        rows = pl.ds(b * 128, 128)
        slots_v[rows] = onehot(j == ((i >> 1) & 31) * 16 + (i >> 7) * 4 + ((i >> 6) & 1) * 2 + (i & 1))
        slotst_v[rows] = onehot(j == ((i >> 2) & 3) * 128 + ((i >> 1) & 1) * 64 + (i >> 4) * 2 + (i & 1))

    pltpu.make_async_copy(qn, qn_v, lsem.at[0]).wait()
    pltpu.make_async_copy(qr, qr_v, lsem.at[1]).wait()
    for hf in range(2):
        parts = []
        for src, wide in ((qn_v, 512), (qr_v, 256)):
            rhs = jnp.concatenate(
                [src[:, c * 2 * wide + hf * wide : c * 2 * wide + hf * wide + wide] for c in range(4)], axis=0
            )
            parts.append((rhs, wide))
        for (rhs, wide), at in zip(parts, (0, 512)):
            for b in range(4):
                got = dot(sel_v[b * 128 : b * 128 + 128], rhs).astype(BF)
                xs[hf, b * 8 : b * 8 + 8, :, at : at + wide] = got.reshape(8, 16, wide)

    def q_latents(par):
        def one(hp, c):
            h = 2 * hp + par
            q = qn_v[:, pl.ds(pl.multiple_of(h * NOPE, NOPE), NOPE)]
            y = dot(q, wuk_v[h]).astype(BF)
            for k in range(TP):
                xlat_v[k, hp] = y[k * OWN : k * OWN + OWN]
            return c

        lax.fori_loop(0, 16, one, 0, unroll=4)
        half = pl.ds(par * 16, 16)
        for k in range(TP):
            for n in range(2):
                z = dot(perm_v[...], xlat_v[k, :, :, n * 256 : n * 256 + 256].reshape(256, 256))
                z = z.astype(BF).reshape(16, 16, 256)
                if k == 0:
                    yrlat[0, :, half, n * 256 : n * 256 + 256] = z
                else:
                    yslat[k - 1, :, half, n * 256 : n * 256 + 256] = z

    for k in range(TP):
        rope = jnp.concatenate(
            [qr_v[k * OWN : k * OWN + OWN, hp * 128 : hp * 128 + 128] for hp in range(16)], axis=0
        )
        z = dot(perm_v[...], rope).astype(BF).reshape(16, 16, 128)
        if k == 0:
            yrrope[0] = z
        else:
            ysrope[k - 1] = z
    ld_wuk.wait()
    q_latents(0)

    def y_to(k):
        return (g, lax.rem(t + k, TP))

    def y_back(k):
        return (g, lax.rem(t + TP - k, TP))

    def y_copy(k, par, c):
        at = (pl.ds(c * 4, 4), pl.ds(par * 16, 16))
        n = (k - 1) * 8 + par * 4 + c
        return pltpu.make_async_remote_copy(
            src_ref=yslat.at[k - 1, at[0], at[1]],
            dst_ref=yrlat.at[k, at[0], at[1]],
            send_sem=yss.at[n], recv_sem=yrs.at[n], device_id=y_to(k), device_id_type=MESH,
        )

    def y_rope_copy(k):
        return pltpu.make_async_remote_copy(
            src_ref=ysrope.at[k - 1], dst_ref=yrrope.at[k],
            send_sem=yrss.at[k - 1], recv_sem=yrrs.at[k - 1], device_id=y_to(k), device_id_type=MESH,
        )

    def x_send(src, dst, ss, rs):
        def one(k, c):
            d = lax.rem(g + k, GROUPS)
            pltpu.make_async_remote_copy(
                src_ref=src.at[d], dst_ref=dst.at[g],
                send_sem=ss, recv_sem=rs, device_id=(d, t), device_id_type=MESH,
            ).start()
            return c

        lax.fori_loop(1, GROUPS, one, 0)

    def x_all(src, dst, ss, rs):
        many = pl.ds(0, GROUPS - 1)
        return pltpu.make_async_remote_copy(
            src_ref=src.at[many], dst_ref=dst.at[many],
            send_sem=ss, recv_sem=rs, device_id=(lax.rem(g + 1, GROUPS), t), device_id_type=MESH,
        )

    pl.semaphore_wait(bar, TP - 1 + GROUPS - 1)
    ropes = [y_rope_copy(k) for k in range(1, TP)]
    for c in ropes:
        c.start()
    ycs = {}
    for c in range(4):
        for k in range(1, TP):
            ycs[k, 0, c] = y_copy(k, 0, c)
            ycs[k, 0, c].start()
    for hf in range(2):
        x_send(xs.at[hf], xr.at[hf], xss.at[hf], xrs.at[hf])
        xr[hf, g] = xs[hf, g]
    q_latents(1)
    for c in range(4):
        for k in range(1, TP):
            ycs[k, 1, c] = y_copy(k, 1, c)
            ycs[k, 1, c].start()

    for p in range(2):
        for c in ld_p[p]:
            c.wait()

        def turn(j, c, p=p):
            at = pl.multiple_of(j * 256, 256)
            kt_v[p, 0:LATENT, pl.ds(at, 256)] = pl_v[p, pl.ds(at, 256), :].T
            return c

        lax.fori_loop(0, PLEN // 256, turn, 0)

    pst[...] = jnp.zeros_like(pst)
    stat_v[...] = jnp.zeros_like(stat_v)
    lane64 = iota((64, 128), 1)
    ld_wuv.wait()

    def prefix_block(hl, par, hf, qb, s, pb, p):
        for n in range(PLEN // 256):
            s[:, n * 256 : n * 256 + 256] = dot(qb[p], kt_v[p, :, n * 256 : n * 256 + 256])
        tops, sums = [], []
        for rc in range(8):
            rows = slice(rc * 32, rc * 32 + 32)
            top = s[rows, 0:128]
            for n in range(1, PLEN // 128):
                top = jnp.maximum(top, s[rows, n * 128 : n * 128 + 128])
            top = jnp.max(top, axis=1, keepdims=True)
            top_b = jnp.broadcast_to(top * SCALE2, (32, 128))
            total = jnp.zeros((32, 128), F32)
            for n in range(PLEN // 256):
                es = []
                for e in range(2):
                    at = n * 256 + e * 128
                    es.append(jnp.exp2(s[rows, at : at + 128] * SCALE2 - top_b))
                    total = total + es[e]
                pb[rows, n * 256 : n * 256 + 256] = jnp.concatenate(es, axis=1).astype(BF)
            tops.append(top)
            sums.append(jnp.sum(total, axis=1, keepdims=True))
        top, total = jnp.concatenate(tops, axis=0), jnp.concatenate(sums, axis=0)
        inv = 1.0 / total
        o = jnp.concatenate(
            [dot(pb[...], pl_v[p, :, n * 256 : n * 256 + 256]) * inv for n in range(2)], axis=1
        ).astype(BF)
        lse = top * SCALE + jnp.log(total)
        hi = lse.astype(BF).astype(F32)
        mid = (lse - hi).astype(BF).astype(F32)
        lo = lse - hi - mid
        for c in range(4):
            rows = slice(c * 64, c * 64 + 64)
            at = pl.ds(c * 128 + p * 64, 64)
            v = dot(o[rows], wuv_v[c * 8 + hl])
            vb[at, pl.ds(pl.multiple_of(hl * VALUE, VALUE), VALUE)] = v.astype(BF)
            row = pst[at]
            for n, part in enumerate((hi, mid, lo)):
                row = jnp.where(lane64 == hl * 3 + n, part[rows], row)
            pst[at] = row

    def prefix_half(hf):
        x_all(xs.at[hf], xr.at[hf], xss.at[hf], xrs.at[hf]).wait_recv()
        for b in range(4):
            for at in range(0, 768, 256):
                cut = xr[hf, :, :, at : at + 256].reshape(512, 256)
                qperm[b * 128 : b * 128 + 128, at : at + 256] = dot(
                    slots_v[b * 128 : b * 128 + 128], cut
                ).astype(BF)

        def pair(i, carry):
            for par, qb in ((0, qb0), (1, qb1)):
                hl = hf * 4 + i * 2 + par
                for c in range(4):
                    q = qperm[c * 128 : c * 128 + 128, pl.ds(pl.multiple_of((i * 2 + par) * 128, 128), 128)]
                    y = dot(q, wuk_v[c * 8 + hl]).astype(BF)
                    r = qperm[c * 128 : c * 128 + 128, pl.ds(pl.multiple_of(512 + i * 128, 128), 128)]
                    lane = iota((128, 128), 1)
                    r = jnp.where((lane < 64) if par == 0 else (lane >= 64), r, jnp.zeros_like(r))
                    for p in range(2):
                        rows = pl.ds(c * 64, 64)
                        qb[p, rows, 0:LATENT] = y[p * 64 : p * 64 + 64]
                        qb[p, rows, LATENT : LATENT + 128] = r[p * 64 : p * 64 + 64]
            for par, qb in ((0, qb0), (1, qb1)):
                hl = hf * 4 + i * 2 + par
                prefix_block(hl, par, hf, qb, s0, pb0, 0)
                prefix_block(hl, par, hf, qb, s1, pb1, 1)
            return carry

        lax.fori_loop(0, 2, pair, 0)

    prefix_half(0)
    for b in range(4):
        z = dot(slotst_v[b * 128 : b * 128 + 128], vb[:, 0:512])
        bs0[b * 8 : b * 8 + 8] = z.astype(BF).reshape(8, 16, 512)
    x_send(bs0, br0, zss.at[0], zrs.at[0])
    br0[g] = bs0[g]

    for c in ld_s:
        c.wait()
    for c in ropes:
        c.wait_recv()
    srow, slane = iota((128, 128), 0), iota((128, 128), 1)

    def suffix_one(r, carry):
        ql = jnp.concatenate([yrlat[k, r] for k in range(TP)], axis=0)
        lane = iota((16, 128), 1)
        parts = []
        for k in range(TP):
            x = yrrope[k, r]
            parts += [jnp.where(lane < 64, x, jnp.zeros_like(x)), jnp.where(lane >= 64, x, jnp.zeros_like(x))]
        kv = sl_v[r]
        s = lax.dot_general(ql, kv, (((1,), (1,)), ((), ())), preferred_element_type=F32)
        s = s + dot(jnp.concatenate(parts, axis=0), skr_v[r])
        live = iota((128, SLEN), 1) < slen[0, t * OWN + r]
        s = jnp.where(live, s, -1e30)
        top = jnp.max(s, axis=1, keepdims=True)
        e = jnp.where(live, jnp.exp2((s - top) * SCALE2), 0.0)
        total = jnp.sum(e, axis=1, keepdims=True)
        o = (dot(e.astype(BF), kv) * (1.0 / total)).astype(BF)
        for k in range(TP):
            for par in range(2):
                at = (k * 2 + par) * 16
                o_v[k, par, r] = o[at : at + 16]
        lse = top * SCALE + jnp.log(total)
        stat_v[...] = jnp.where(slane == (srow >> 5) * OWN + r, lse, stat_v[...])
        return carry

    for c in range(4):
        for par in range(2):
            for k in range(1, TP):
                ycs[k, par, c].wait_recv()
        lax.fori_loop(c * 4, c * 4 + 4, suffix_one, 0, unroll=2)

    def yb_copy(k, q):
        at = pl.ds(q * 4, 4)
        n = (k - 1) * 4 + q
        return pltpu.make_async_remote_copy(
            src_ref=ybs.at[k - 1, at], dst_ref=ybr.at[k, at],
            send_sem=bss.at[n], recv_sem=brs.at[n], device_id=y_back(k), device_id_type=MESH,
        )

    def yb_stat_copy(k):
        return pltpu.make_async_remote_copy(
            src_ref=ybs_st.at[k - 1], dst_ref=ybr_st.at[k],
            send_sem=bsts.at[k - 1], recv_sem=brts.at[k - 1], device_id=y_back(k), device_id_type=MESH,
        )

    for k in range(TP):
        part = stat_v[k * 32 : k * 32 + 32]
        if k == 0:
            ybr_st[0] = part
        else:
            ybs_st[k - 1] = part
    stats = [yb_stat_copy(k) for k in range(1, TP)]
    for c in stats:
        c.start()
    backs = {}
    for q in range(4):
        for k in range(TP):
            for par in range(2):
                for n in range(2):
                    cut = o_v[k, par, :, :, n * 256 : n * 256 + 256].reshape(256, 256)
                    z = dot(perm_v[q * 64 : q * 64 + 64], cut).astype(BF).reshape(4, 16, 256)
                    if k == 0:
                        ybr[0, q * 4 : q * 4 + 4, par, :, n * 256 : n * 256 + 256] = z
                    else:
                        ybs[k - 1, q * 4 : q * 4 + 4, par, :, n * 256 : n * 256 + 256] = z
            if k:
                backs[k, q] = yb_copy(k, q)
                backs[k, q].start()

    prefix_half(1)
    vb[:, 1024 : 1024 + STATS] = pst[...].astype(BF)
    for b in range(4):
        z = dot(slotst_v[b * 128 : b * 128 + 128], vb[:, 512 : 1024 + STATS])
        bs1[b * 8 : b * 8 + 8] = z.astype(BF).reshape(8, 16, 512 + STATS)
    x_send(bs1, br1, zss.at[1], zrs.at[1])
    br1[g] = bs1[g]

    x_all(bs0, br0, zss.at[0], zrs.at[0]).wait_recv()
    x_all(bs1, br1, zss.at[1], zrs.at[1]).wait_recv()
    for c in stats:
        c.wait_recv()
    st = ybr_st[0] + ybr_st[1] + ybr_st[2] + ybr_st[3]
    st = jnp.concatenate([st, jnp.zeros((96, 128), F32)], axis=0).T
    outs = []
    for q in range(4):
        rows = selt_v[q * 64 : q * 64 + 64]
        pv = (dot(rows, br0[...].reshape(512, 512)), dot(rows, br1[...].reshape(512, 512 + STATS)))
        for k in range(1, TP):
            backs[k, q].wait_recv()
        for hl in range(8):
            h = q * 8 + hl
            hp, par = h // 2, h % 2
            lhs = jnp.concatenate([ybr[k, hp, par] for k in range(TP)], axis=0)
            sv = dot(lhs, wuv_v[h]).astype(BF).astype(F32)
            at = (hl % 4) * 128
            prefix = pv[hl // 4][:, at : at + 128]
            lp = pv[1][:, 512 + hl * 3 : 512 + hl * 3 + 1]
            for n in range(1, 3):
                lp = lp + pv[1][:, 512 + hl * 3 + n : 512 + hl * 3 + n + 1]
            ls = st[0:64, par * 16 + hp : par * 16 + hp + 1]
            top = jnp.maximum(lp, ls)
            a, b = jnp.exp(lp - top), jnp.exp(ls - top)
            inv = 1.0 / (a + b)
            out_v[:, h * 128 : h * 128 + 128] = ((a * inv) * prefix + (b * inv) * sv).astype(BF)
        for k in range(TP):
            c = pltpu.make_async_copy(
                out_v.at[pl.ds(k * OWN, OWN), pl.ds(q * 1024, 1024)],
                out.at[pl.ds(rel(k), OWN), pl.ds(q * 1024, 1024)],
                osem.at[q * 4 + k],
            )
            c.start()
            outs.append(c)
    for c in outs:
        c.wait()
    for c in (*ropes, *ycs.values(), *backs.values(), *stats):
        c.wait_send()
    for hf in range(2):
        x_all(xs.at[hf], xr.at[hf], xss.at[hf], xrs.at[hf]).wait_send()
    x_all(bs0, br0, zss.at[0], zrs.at[0]).wait_send()
    x_all(bs1, br1, zss.at[1], zrs.at[1]).wait_send()


def local(qn, qr, wuk, wuv, plat, prope, slat, srope, slen, named, slot):
    rp = jnp.broadcast_to(jnp.tile(named, 2)[None], (8, 128))
    ps = jnp.broadcast_to(jnp.tile(slot, 2)[None], (8, 128))
    hbm = pl.BlockSpec(memory_space=pl.ANY)
    vmem = pl.BlockSpec(memory_space=pltpu.VMEM)
    smem = pl.BlockSpec(memory_space=pltpu.SMEM)

    def b(*shape):
        return pltpu.VMEM(shape, BF)

    def f(*shape):
        return pltpu.VMEM(shape, F32)

    def sem(n):
        return pltpu.SemaphoreType.DMA((n,))

    return pl.pallas_call(
        kernel,
        out_shape=jax.ShapeDtypeStruct((REQS, HEADS * VALUE), BF),
        in_specs=[hbm] * 8 + [vmem, vmem, smem],
        out_specs=hbm,
        scratch_shapes=[
            b(64, 4096), b(64, 2048), b(32, 128, 512), b(32, 512, 128), b(2, 2048, 512), b(2, 640, 2048),
            b(16, 256, 512), b(16, 128, 256),
            b(512, 256), b(256, 512), b(256, 256), b(512, 512), b(512, 512),
            b(4, 16, 16, 512), b(3, 16, 32, 512), b(4, 16, 32, 512), b(3, 16, 16, 128), b(4, 16, 16, 128),
            b(4, 2, 16, 16, 512), b(3, 16, 2, 16, 512), b(4, 16, 2, 16, 512),
            f(128, 128), f(3, 32, 128), f(4, 32, 128),
            b(2, 32, 16, 768), b(2, 32, 16, 768), b(512, 768), b(512, 1024 + STATS), f(512, 128),
            b(32, 16, 512), b(32, 16, 512), b(32, 16, 512 + STATS), b(32, 16, 512 + STATS),
            b(2, 256, 640), b(2, 256, 640), f(256, 2048), f(256, 2048), b(256, 2048), b(256, 2048),
            b(64, 4096),
            sem(13), sem(16), sem(24), sem(24), sem(3), sem(3), sem(12), sem(12), sem(3), sem(3),
            sem(2), sem(2), sem(2), sem(2),
        ],
        compiler_params=pltpu.CompilerParams(
            collective_id=0, has_side_effects=True, vmem_limit_bytes=67043328
        ),
        name="attend",
    )(qn, qr, wuk, wuv, plat, prope, slat, srope, rp, ps, slen)


def solution(mesh):
    in_specs = (
        P("grp", "tp"), P("grp", "tp"), P("tp", None, None), P("tp", None, None),
        P("grp", None, None), P("grp", None, None), P(("grp", "tp"), None, None), P(("grp", "tp"), None, None),
        P("grp", None), P("grp"), P(),
    )
    return jax.shard_map(local, mesh=mesh, in_specs=in_specs, out_specs=P("grp", "tp"), check_vma=False)
```

```python
import math

import jax
import jax.numpy as jnp
from jax import lax
from jax.experimental import pallas as pl
from jax.experimental.pallas import tpu as pltpu
from jax.sharding import PartitionSpec as P

MESH = pl.DeviceIdType.MESH
BF, F32, I32 = jnp.bfloat16, jnp.float32, jnp.int32
LATENT, ROPE, NOPE, VALUE = 512, 64, 128, 128
PLEN, SLEN = 2048, 256
HEADS, REQS, OWN, GROUPS, TP = 32, 64, 16, 32, 4
SCALE = 1.0 / math.sqrt(NOPE + ROPE)
SCALE2 = SCALE * math.log2(math.e)
QUARTERS = 4
STATS = 128


def dot(a, b):
    return jnp.dot(a, b, preferred_element_type=F32)


def iota(shape, dim):
    return lax.broadcasted_iota(I32, shape, dim)


def onehot(mask):
    return jnp.where(mask, 1.0, 0.0).astype(BF)


def kernel(
    qn, qr, wuk, wuv, plat, prope, slat, srope, rp, ps, slen, out,
    qn_v, qr_v, wuk_v, wuv_v, pl_v, kt_v, sl_v, skr_v,
    sel_v, selt_v, perm_v, permb_v, slots_v, slotst_v,
    xlat_v, yslat, yrlat, ysrope, yrrope, o_v, ybs, ybr, stat_v, ybs_st, ybr_st,
    xs, xr, qp, vq, pst, bs, br, bs_st, br_st,
    qb, sc, pb, ob, ss, es, pv_v, sv_v, out_v,
    lsem, osem, yss, yrs, yrss, yrrs, bss, brs, bsts, brts, xss, xrs, zss, zrs,
):
    g, t = lax.axis_index("grp"), lax.axis_index("tp")
    def rel(k):
        return pl.multiple_of(lax.rem(t + k, TP) * OWN, OWN)

    for k in range(TP):
        rows = pl.ds(k * OWN, OWN)
        pltpu.make_async_copy(qn.at[pl.ds(rel(k), OWN)], qn_v.at[rows], lsem.at[0]).start()
        pltpu.make_async_copy(qr.at[pl.ds(rel(k), OWN)], qr_v.at[rows], lsem.at[1]).start()
    loads = [(wuk, wuk_v)]
    for p in range(2):
        loads.append((plat.at[p], pl_v.at[p]))
        for b in range(2):
            loads.append((prope.at[p], kt_v.at[p, pl.ds(LATENT + b * ROPE, ROPE)]))
    loads.append((slat, sl_v))
    for b in range(2):
        loads.append((srope, skr_v.at[:, pl.ds(b * ROPE, ROPE)]))
    loads.append((wuv, wuv_v))
    copies = [pltpu.make_async_copy(a, b, lsem.at[2 + i]) for i, (a, b) in enumerate(loads)]
    copies[0].start()
    bar = pltpu.get_barrier_semaphore()
    for k in range(1, TP):
        pl.semaphore_signal(bar, inc=1, device_id=(g, lax.rem(t + k, TP)), device_id_type=MESH)

    def greet(k, c):
        pl.semaphore_signal(bar, inc=1, device_id=(lax.rem(g + k, GROUPS), t), device_id_type=MESH)
        return c

    lax.fori_loop(1, GROUPS, greet, 0)

    for c in copies[1:]:
        c.start()
    ld_wuk, ld_p, ld_s, ld_wuv = copies[0], (copies[1:4], copies[4:7]), copies[7:10], copies[10]

    i, j = iota((256, 256), 0), iota((256, 256), 1)
    perm_v[...] = onehot(j == (i & 15) * 16 + (i >> 4))

    def q_latents(par):
        def one(hp, c):
            h = 2 * hp + par
            q = qn_v[:, pl.ds(pl.multiple_of(h * NOPE, NOPE), NOPE)]
            y = dot(q, wuk_v[h]).astype(BF)
            for k in range(TP):
                xlat_v[k, hp] = y[k * OWN : k * OWN + OWN]
            return c

        lax.fori_loop(0, 16, one, 0, unroll=4)
        half = pl.ds(par * 16, 16)
        for k in range(TP):
            for n in range(2):
                z = dot(perm_v[...], xlat_v[k, :, :, n * 256 : n * 256 + 256].reshape(256, 256))
                z = z.astype(BF).reshape(16, 16, 256)
                if k == 0:
                    yrlat[0, :, half, n * 256 : n * 256 + 256] = z
                else:
                    yslat[k - 1, :, half, n * 256 : n * 256 + 256] = z

    with jax.named_scope("wait_q"):
        pltpu.make_async_copy(qn, qn_v, lsem.at[0]).wait()
        pltpu.make_async_copy(qr, qr_v, lsem.at[1]).wait()
    with jax.named_scope("ropes"):
        for k in range(TP):
            rope = jnp.concatenate(
                [qr_v[k * OWN : k * OWN + OWN, hp * 128 : hp * 128 + 128] for hp in range(16)], axis=0
            )
            z = dot(perm_v[...], rope).astype(BF).reshape(16, 16, 128)
            if k == 0:
                yrrope[0] = z
            else:
                ysrope[k - 1] = z
    ld_wuk.wait()
    with jax.named_scope("qlat0"):
        q_latents(0)

    def y_to(k):
        return (g, lax.rem(t + k, TP))

    def y_back(k):
        return (g, lax.rem(t + TP - k, TP))

    def y_copy(k, par, c):
        at = (pl.ds(c * 4, 4), pl.ds(par * 16, 16))
        n = (k - 1) * 8 + par * 4 + c
        return pltpu.make_async_remote_copy(
            src_ref=yslat.at[k - 1, at[0], at[1]],
            dst_ref=yrlat.at[k, at[0], at[1]],
            send_sem=yss.at[n], recv_sem=yrs.at[n], device_id=y_to(k), device_id_type=MESH,
        )

    def y_rope_copy(k):
        return pltpu.make_async_remote_copy(
            src_ref=ysrope.at[k - 1], dst_ref=yrrope.at[k],
            send_sem=yrss.at[k - 1], recv_sem=yrrs.at[k - 1], device_id=y_to(k), device_id_type=MESH,
        )

    def x_send(src, dst, ss, rs):
        def one(k, c):
            d = lax.rem(g + k, GROUPS)
            pltpu.make_async_remote_copy(
                src_ref=src.at[d], dst_ref=dst.at[g],
                send_sem=ss, recv_sem=rs, device_id=(d, t), device_id_type=MESH,
            ).start()
            return c

        lax.fori_loop(1, GROUPS, one, 0)
        dst[g] = src[g]

    def x_all(src, dst, ss, rs):
        many = pl.ds(0, GROUPS - 1)
        return pltpu.make_async_remote_copy(
            src_ref=src.at[many], dst_ref=dst.at[many],
            send_sem=ss, recv_sem=rs, device_id=(lax.rem(g + 1, GROUPS), t), device_id_type=MESH,
        )

    def forward(i):
        return xs.at[i], xr.at[i], xss.at[i], xrs.at[i]

    def backward(i):
        return bs.at[i], br.at[i], zss.at[i], zrs.at[i]

    back_stats = (bs_st, br_st, zss.at[QUARTERS], zrs.at[QUARTERS])

    with jax.named_scope("barrier"):
        pl.semaphore_wait(bar, TP - 1 + GROUPS - 1)
    ropes = [y_rope_copy(k) for k in range(1, TP)]
    for c in ropes:
        c.start()
    for k in range(1, TP):
        y_copy(k, 0, 0).start()
    with jax.named_scope("route"):
        sq = (128, 128)
        first = iota(sq, 0)
        lane1 = iota((1, 128), 1) & 63
        slot = jnp.zeros((1, 128), I32)
        for j in range(REQS):
            slot = jnp.where(lane1 == j, ps[rp[lax.rem(t * OWN + j, REQS)]], slot)
        slot = slot.astype(F32)
        slot_b = jnp.broadcast_to(slot, sq)
        before = first < (iota(sq, 1) & 63)
        rank = jnp.sum(jnp.where(before & (slot_b.T == slot_b), 1.0, 0.0), axis=0, keepdims=True)
        buf = jnp.broadcast_to(2.0 * slot + rank, sq)
        buf_r = buf.astype(I32)
        buf_c = buf.T.astype(I32)
        for b in range(4):
            i, j = iota(sq, 0) + b * 128, iota(sq, 1)
            key, col = (i >> 4) * 4 + (i & 3), (i >> 2) & 3
            for e in range(2):
                sel_v[b * 128 : b * 128 + 128, e * 128 : e * 128 + 128] = onehot(
                    (key == buf_r) & (col == ((j + e * 128) >> 6))
                )

    with jax.named_scope("place"):
        for hf in range(QUARTERS):
            for src, wide, at in ((qn_v, 256, 0), (qr_v, 128, 256)):
                rhs = jnp.concatenate(
                    [src[:, (c * 4 + hf) * wide : (c * 4 + hf) * wide + wide] for c in range(4)], axis=0
                )
                for b in range(4):
                    got = dot(sel_v[b * 128 : b * 128 + 128], rhs).astype(BF)
                    xs[hf, b * 8 : b * 8 + 8, :, at : at + wide] = got.reshape(8, 16, wide)
            x_send(*forward(hf))
    with jax.named_scope("qlat1"):
        q_latents(1)
    for c in range(4):
        for par in range(2):
            for k in range(1, TP):
                if c or par:
                    y_copy(k, par, c).start()

    with jax.named_scope("masks"):
        for b in range(4):
            i, j = iota((128, 512), 0) + b * 128, iota((128, 512), 1)
            rows = pl.ds(b * 128, 128)
            slots_v[rows] = onehot(j == ((i >> 1) & 31) * 16 + (i >> 7) * 4 + ((i >> 6) & 1) * 2 + (i & 1))
            slotst_v[rows] = onehot(
                j == ((i >> 2) & 3) * 128 + ((i >> 1) & 1) * 64 + (i >> 4) * 2 + (i & 1)
            )
            i, j = iota(sq, 0), iota(sq, 1) + b * 128
            key, col = (j >> 4) * 4 + (j & 3), (j >> 2) & 3
            for e in range(2):
                selt_v[e * 128 : e * 128 + 128, b * 128 : b * 128 + 128] = onehot(
                    (key == buf_c) & (col == ((i + e * 128) >> 6))
                )
        i, j = iota((256, 256), 0), iota((256, 256), 1)
        permb_v[...] = onehot(j == (i & 7) * 32 + ((i >> 3) & 1) * 16 + (i >> 4))

    with jax.named_scope("turn"):
        for p in range(2):
            for c in ld_p[p]:
                c.wait()

            def turn(j, c, p=p):
                at = pl.multiple_of(j * 256, 256)
                kt_v[p, 0:LATENT, pl.ds(at, 256)] = pl_v[p, pl.ds(at, 256), :].T
                return c

            lax.fori_loop(0, PLEN // 256, turn, 0)

    pst[...] = jnp.zeros_like(pst)
    stat_v[...] = jnp.zeros_like(stat_v)
    lane64 = iota((64, 128), 1)
    with jax.named_scope("loads"):
        ld_wuv.wait()
        for c in ld_s:
            c.wait()

    def scores(b, n):
        at = pl.ds(n * 256, 256)
        sc[b % 2, :, at] = dot(qb[b], kt_v[b % 2, :, at])

    def weigh(b, n):
        rows = slice(n * 32, n * 32 + 32)
        s = sc.at[b % 2]
        top = s[rows, 0:128]
        for m in range(1, PLEN // 128):
            top = jnp.maximum(top, s[rows, m * 128 : m * 128 + 128])
        top = jnp.max(top, axis=1, keepdims=True)
        top_b = jnp.broadcast_to(top * SCALE2, (32, 128))
        total = jnp.zeros((32, 128), F32)
        for m in range(PLEN // 256):
            e = [
                jnp.exp2(s[rows, at : at + 128] * SCALE2 - top_b)
                for at in (m * 256, m * 256 + 128)
            ]
            total = total + e[0] + e[1]
            pb[b % 2, rows, m * 256 : m * 256 + 256] = jnp.concatenate(e, axis=1).astype(BF)
        return top, jnp.sum(total, axis=1, keepdims=True)

    def values(b, n, inv):
        at = pl.ds(n * 256, 256)
        ob[b % 2, :, at] = (dot(pb[b % 2], pl_v[b % 2, :, at]) * inv).astype(BF)

    def quarter(i):
        with jax.named_scope("wait_x"):
            x_all(*forward(i)).wait_recv()
        for b in range(4):
            for at, wide in ((0, 256), (256, 128)):
                cut = xr[i, :, :, at : at + wide].reshape(512, wide)
                qp[b * 128 : b * 128 + 128, at : at + wide] = dot(
                    slots_v[b * 128 : b * 128 + 128], cut
                ).astype(BF)
        lane = iota((128, 128), 1)
        for par in range(2):
            for c in range(4):
                rows = slice(c * 128, c * 128 + 128)
                y = dot(qp[rows, par * 128 : par * 128 + 128], wuk_v[c * 8 + 2 * i + par]).astype(BF)
                r = qp[rows, 256:384]
                r = jnp.where((lane < 64) if par == 0 else (lane >= 64), r, jnp.zeros_like(r))
                for p in range(2):
                    qb[par * 2 + p, c * 64 : c * 64 + 64, 0:LATENT] = y[p * 64 : p * 64 + 64]
                    qb[par * 2 + p, c * 64 : c * 64 + 64, LATENT : LATENT + 128] = r[p * 64 : p * 64 + 64]
        inv = {}
        for step in range(6):
            a, b, c = step, step - 1, step - 2
            parts = []
            for n in range(8):
                if a < 4:
                    scores(a, n)
                if 0 <= b < 4:
                    parts.append(weigh(b, n))
                if 0 <= c and n % 4 == 0:
                    values(c, n // 4, inv[c])
            if 0 <= b < 4:
                top = jnp.concatenate([x[0] for x in parts], axis=0)
                total = jnp.concatenate([x[1] for x in parts], axis=0)
                inv[b] = 1.0 / total
                lse = top * SCALE + jnp.log(total)
                hi = lse.astype(BF).astype(F32)
                mid = (lse - hi).astype(BF).astype(F32)
                lo = lse - hi - mid
                for e in range(4):
                    at = slice(e * 128 + (b % 2) * 64, e * 128 + (b % 2) * 64 + 64)
                    row = pst[at]
                    for n, part in enumerate((hi, mid, lo)):
                        at_lane = n * 32 + (b // 2) * 16 + e * 4 + i
                        row = jnp.where(lane64 == at_lane, part[e * 64 : e * 64 + 64], row)
                    pst[at] = row
            if c in (1, 3):
                par = c // 2
                for e in range(4):
                    rows = slice(e * 64, e * 64 + 64)
                    lhs = jnp.concatenate([ob[0, rows], ob[1, rows]], axis=0)
                    v = dot(lhs, wuv_v[e * 8 + 2 * i + par])
                    vq[e * 128 : e * 128 + 128, par * 128 : par * 128 + 128] = v.astype(BF)
        for b in range(4):
            z = dot(slotst_v[b * 128 : b * 128 + 128], vq[...])
            bs[i, b * 8 : b * 8 + 8] = z.astype(BF).reshape(8, 16, 256)
        x_send(*backward(i))

    srow, slane = iota((128, 128), 0), iota((128, 128), 1)

    def suffix(c):
        with jax.named_scope("wait_y"):
            for par in range(2):
                for k in range(1, TP):
                    y_copy(k, par, c).wait_recv()
        lane = iota((16, 128), 1)
        spos = iota((128, SLEN), 1)

        def match(j):
            r = c * 4 + j
            ql = jnp.concatenate([yrlat[k, r] for k in range(TP)], axis=0)
            parts = []
            for k in range(TP):
                x = yrrope[k, r]
                zero = jnp.zeros_like(x)
                parts += [jnp.where(lane < 64, x, zero), jnp.where(lane >= 64, x, zero)]
            s = lax.dot_general(ql, sl_v[r], (((1,), (1,)), ((), ())), preferred_element_type=F32)
            ss[j] = s + dot(jnp.concatenate(parts, axis=0), skr_v[r])

        def soft(j):
            r = c * 4 + j
            live = spos < slen[0, t * OWN + r]
            s = jnp.where(live, ss[j], -1e30)
            top = jnp.max(s, axis=1, keepdims=True)
            e = jnp.where(live, jnp.exp2((s - top) * SCALE2), 0.0)
            total = jnp.sum(e, axis=1, keepdims=True)
            es[j] = e.astype(BF)
            lse = top * SCALE + jnp.log(total)
            stat_v[...] = jnp.where(slane == (srow >> 5) * OWN + r, lse, stat_v[...])
            return 1.0 / total

        def mixed(j, inv):
            r = c * 4 + j
            for n in range(2):
                at = pl.ds(n * 256, 256)
                o = (dot(es[j], sl_v[r, :, at]) * inv).astype(BF)
                for k in range(TP):
                    o_v[k, r, :, at] = o[k * 32 : k * 32 + 32]

        inv = {}
        for step in range(6):
            if step < 4:
                match(step)
            if 0 <= step - 1 < 4:
                inv[step - 1] = soft(step - 1)
            if 0 <= step - 2:
                mixed(step - 2, inv[step - 2])

    def yb_copy(k, rh, q):
        at = pl.ds(q * 4, 4)
        n = (k - 1) * 8 + rh * 4 + q
        return pltpu.make_async_remote_copy(
            src_ref=ybs.at[k - 1, rh, at], dst_ref=ybr.at[k, rh, at],
            send_sem=bss.at[n], recv_sem=brs.at[n], device_id=y_back(k), device_id_type=MESH,
        )

    def yb_stat_copy(k):
        return pltpu.make_async_remote_copy(
            src_ref=ybs_st.at[k - 1], dst_ref=ybr_st.at[k],
            send_sem=bsts.at[k - 1], recv_sem=brts.at[k - 1], device_id=y_back(k), device_id_type=MESH,
        )

    def return_half(rh):
        for k in (1, 2, 3, 0):
            for n in range(2):
                cut = o_v[k, pl.ds(rh * 8, 8), :, n * 256 : n * 256 + 256].reshape(256, 256)
                z = dot(permb_v[...], cut).astype(BF).reshape(16, 16, 256)
                if k == 0:
                    ybr[0, rh, :, :, n * 256 : n * 256 + 256] = z
                else:
                    ybs[k - 1, rh, :, :, n * 256 : n * 256 + 256] = z
            if k == 3:
                for q in range(4):
                    for m in range(1, TP):
                        yb_copy(m, rh, q).start()

    with jax.named_scope("wait_rope"):
        for c in ropes:
            c.wait_recv()

    def attend(j, carry):
        with jax.named_scope("quarter"):
            quarter(j)
        with jax.named_scope("suffix"):
            suffix(j)
        return carry

    def attend_suffix(j, carry):
        with jax.named_scope("suffix"):
            suffix(j)
        return carry

    def attend_prefix(j, carry):
        with jax.named_scope("quarter"):
            quarter(j)
        return carry

    lax.fori_loop(0, 2, attend, 0)
    with jax.named_scope("yback"):
        return_half(0)
    lax.fori_loop(2, 4, attend_suffix, 0)
    for k in range(TP):
        part = stat_v[k * 32 : k * 32 + 32]
        if k == 0:
            ybr_st[0] = part
        else:
            ybs_st[k - 1] = part
    stats = [yb_stat_copy(k) for k in range(1, TP)]
    for c in stats:
        c.start()
    with jax.named_scope("yback"):
        return_half(1)
    lax.fori_loop(2, 4, attend_prefix, 0)
    for b in range(4):
        z = dot(slotst_v[b * 128 : b * 128 + 128], pst[...].astype(BF))
        bs_st[b * 8 : b * 8 + 8] = z.astype(BF).reshape(8, 16, STATS)
    x_send(*back_stats)

    def prefix_part(i):
        with jax.named_scope("wait_x_back"):
            x_all(*backward(i)).wait_recv()
        pv_v[i] = dot(selt_v[...], br[i].reshape(512, 256))

    def suffix_part(q):
        with jax.named_scope("wait_yback"):
            for rh in range(2):
                for k in range(1, TP):
                    yb_copy(k, rh, q).wait_recv()
        for hp in range(q * 4, q * 4 + 4):
            lhs = jnp.concatenate([ybr[k, rh, hp] for k in range(TP) for rh in range(2)], axis=0)
            rhs = jnp.concatenate([wuv_v[2 * hp], wuv_v[2 * hp + 1]], axis=1)
            sv = dot(lhs, rhs)
            for par in range(2):
                h = 2 * hp + par
                sv_v[:, h * 128 : h * 128 + 128] = jnp.concatenate(
                    [sv[e * 16 + par * 8 : e * 16 + par * 8 + 8, par * 128 : par * 128 + 128] for e in range(8)],
                    axis=0,
                ).astype(BF)

    with jax.named_scope("parts"):
        for i in range(QUARTERS - 1):
            prefix_part(i)
            suffix_part(i)
    with jax.named_scope("wait_stats"):
        x_all(*back_stats).wait_recv()
        for c in stats:
            c.wait_recv()
    st = ybr_st[0] + ybr_st[1] + ybr_st[2] + ybr_st[3]
    ls = jnp.concatenate([st, jnp.zeros((96, 128), F32)], axis=0).T[0:64]
    lp = jnp.zeros((64, 128), F32)
    for c in range(4):
        lp = lp + dot(selt_v[c * 64 : c * 64 + 64], br_st[...].reshape(512, STATS))
    lp = lp + pltpu.roll(lp, 96, 1) + pltpu.roll(lp, 64, 1)
    top = jnp.maximum(lp, ls)
    a, b = jnp.exp(lp - top), jnp.exp(ls - top)
    inv = 1.0 / (a + b)
    a, b = a * inv, b * inv
    with jax.named_scope("last"):
        prefix_part(QUARTERS - 1)
        suffix_part(3)
    outs = []
    for q in range(4):
        with jax.named_scope("finish"):
            for hl in range(8):
                h, i, par = q * 8 + hl, hl // 2, hl % 2
                at, col = slice(h * 128, h * 128 + 128), par * 16 + h // 2
                prefix = pv_v[i, q * 64 : q * 64 + 64, par * 128 : par * 128 + 128]
                own = sv_v[:, at].astype(F32)
                out_v[:, at] = (a[:, col : col + 1] * prefix + b[:, col : col + 1] * own).astype(BF)
            for k in range(TP):
                c = pltpu.make_async_copy(
                    out_v.at[pl.ds(k * OWN, OWN), pl.ds(q * 1024, 1024)],
                    out.at[pl.ds(rel(k), OWN), pl.ds(q * 1024, 1024)],
                    osem.at[q * 4 + k],
                )
                c.start()
                outs.append(c)
    with jax.named_scope("wait_sends"):
        for k in range(1, TP):
            for c in range(4):
                for par in range(2):
                    y_copy(k, par, c).wait_send()
                    yb_copy(k, par, c).wait_send()
        for c in (*ropes, *stats):
            c.wait_send()
        for i in range(QUARTERS):
            x_all(*forward(i)).wait_send()
            x_all(*backward(i)).wait_send()
        x_all(*back_stats).wait_send()
    with jax.named_scope("waitout"):
        for c in outs:
            c.wait()


def local(qn, qr, wuk, wuv, plat, prope, slat, srope, slen, named, slot):
    hbm = pl.BlockSpec(memory_space=pl.ANY)
    smem = pl.BlockSpec(memory_space=pltpu.SMEM)

    def b(*shape):
        return pltpu.VMEM(shape, BF)

    def f(*shape):
        return pltpu.VMEM(shape, F32)

    def sem(n):
        return pltpu.SemaphoreType.DMA((n,))

    return pl.pallas_call(
        kernel,
        out_shape=jax.ShapeDtypeStruct((REQS, HEADS * VALUE), BF),
        in_specs=[hbm] * 8 + [smem] * 3,
        out_specs=hbm,
        scratch_shapes=[
            b(64, 4096), b(64, 2048), b(32, 128, 512), b(32, 512, 128), b(2, 2048, 512), b(2, 640, 2048),
            b(16, 256, 512), b(16, 128, 256),
            b(512, 256), b(256, 512), b(256, 256), b(256, 256), b(512, 512), b(512, 512),
            b(4, 16, 16, 512), b(3, 16, 32, 512), b(4, 16, 32, 512), b(3, 16, 16, 128), b(4, 16, 16, 128),
            b(4, 16, 32, 512), b(3, 2, 16, 16, 512), b(4, 2, 16, 16, 512),
            f(128, 128), f(3, 32, 128), f(4, 32, 128),
            b(4, 32, 16, 384), b(4, 32, 16, 384), b(512, 384), b(512, 256), f(512, 128),
            b(4, 32, 16, 256), b(4, 32, 16, 256), b(32, 16, STATS), b(32, 16, STATS),
            b(4, 256, 640), f(2, 256, 2048), b(2, 256, 2048), b(2, 256, 512),
            f(4, 128, 256), b(4, 128, 256), f(4, 256, 256), b(64, 4096), b(64, 4096),
            sem(13), sem(16), sem(24), sem(24), sem(3), sem(3), sem(24), sem(24), sem(3), sem(3),
            sem(4), sem(4), sem(5), sem(5),
        ],
        compiler_params=pltpu.CompilerParams(
            collective_id=0, has_side_effects=True, vmem_limit_bytes=67043328
        ),
        name="attend",
    )(qn, qr, wuk, wuv, plat, prope, slat, srope, named, slot, slen)


def solution(mesh):
    in_specs = (
        P("grp", "tp"), P("grp", "tp"), P("tp", None, None), P("tp", None, None),
        P("grp", None, None), P("grp", None, None), P(("grp", "tp"), None, None), P(("grp", "tp"), None, None),
        P("grp", None), P("grp"), P(),
    )
    return jax.shard_map(local, mesh=mesh, in_specs=in_specs, out_specs=P("grp", "tp"), check_vma=False)
```

```python
import math

import jax
import jax.numpy as jnp
from jax import lax
from jax.experimental import pallas as pl
from jax.experimental.pallas import tpu as pltpu
from jax.sharding import PartitionSpec as P

MESH = pl.DeviceIdType.MESH
BF, F32, I32 = jnp.bfloat16, jnp.float32, jnp.int32
LATENT, ROPE, NOPE, VALUE = 512, 64, 128, 128
PLEN, SLEN = 2048, 256
HEADS, REQS, OWN, GROUPS, TP = 32, 64, 16, 32, 4
SCALE = 1.0 / math.sqrt(NOPE + ROPE)
SCALE2 = SCALE * math.log2(math.e)
QUARTERS = 4
STATS = 128


def dot(a, b):
    return jnp.dot(a, b, preferred_element_type=F32)


def iota(shape, dim):
    return lax.broadcasted_iota(I32, shape, dim)


def onehot(mask):
    return jnp.where(mask, 1.0, 0.0).astype(BF)


def kernel(
    qn, qr, wuk, wuv, plat, prope, slat, srope, rp, ps, slen, out,
    qn_v, qr_v, wuk_v, wuv_v, pl_v, kt_v, sl_v, skr_v,
    sel_v, selt_v, perm_v, permb_v, slots_v, slotst_v,
    xlat_v, yslat, yrlat, ysrope, yrrope, o_v, ybs, ybr, stat_v, ybs_st, ybr_st,
    xs, xr, qp, vq, pst, bs, br, bs_c, br_c, bs_a, br_a, bs_b, br_b,
    qb, sc, pb, ob, ss, es, pv_v, sv_v, out_v,
    lsem, osem, yss, yrs, yrss, yrrs, bss, brs, bsts, brts, xss, xrs, zss, zrs,
):
    g, t = lax.axis_index("grp"), lax.axis_index("tp")
    def rel(k):
        return pl.multiple_of(lax.rem(t + k, TP) * OWN, OWN)

    for k in range(TP):
        rows = pl.ds(k * OWN, OWN)
        pltpu.make_async_copy(qn.at[pl.ds(rel(k), OWN)], qn_v.at[rows], lsem.at[0]).start()
        pltpu.make_async_copy(qr.at[pl.ds(rel(k), OWN)], qr_v.at[rows], lsem.at[1]).start()
    loads = [(wuk.at[:, b], wuk_v.at[:, b]) for b in range(2)]
    for p in range(2):
        loads.append((plat.at[p], pl_v.at[p]))
        for b in range(2):
            loads.append((prope.at[p], kt_v.at[p, pl.ds(LATENT + b * ROPE, ROPE)]))
    loads.append((slat, sl_v))
    for b in range(2):
        loads.append((srope, skr_v.at[:, pl.ds(b * ROPE, ROPE)]))
    loads.append((wuv, wuv_v))
    copies = [pltpu.make_async_copy(a, b, lsem.at[2 + i]) for i, (a, b) in enumerate(loads)]
    copies[0].start()
    bar = pltpu.get_barrier_semaphore()
    for k in range(1, TP):
        pl.semaphore_signal(bar, inc=1, device_id=(g, lax.rem(t + k, TP)), device_id_type=MESH)

    for k in range(1, GROUPS):
        pl.semaphore_signal(bar, inc=1, device_id=(lax.rem(g + k, GROUPS), t), device_id_type=MESH)

    for c in copies[1:]:
        c.start()
    ld_wuk, ld_p, ld_s, ld_wuv = copies[0:2], copies[2:8], copies[8:11], copies[11]

    i, j = iota((256, 256), 0), iota((256, 256), 1)
    perm_v[...] = onehot(j == (i & 15) * 16 + (i >> 4))

    def q_latents(par):
        def one(hp, c):
            h = 2 * hp + par
            q = qn_v[:, pl.ds(pl.multiple_of(h * NOPE, NOPE), NOPE)]
            y = dot(q, wuk_v[hp, par]).astype(BF)
            for k in range(TP):
                xlat_v[k, hp] = y[k * OWN : k * OWN + OWN]
            if par:
                p, at = hp // 8, pl.multiple_of((hp % 8) * 256, 256)
                kt_v[p, 0:LATENT, pl.ds(at, 256)] = pl_v[p, pl.ds(at, 256), :].T
            return c

        lax.fori_loop(0, 16, one, 0, unroll=4)
        half = pl.ds(par * 16, 16)
        for k in range(TP):
            for n in range(2):
                z = dot(perm_v[...], xlat_v[k, :, :, n * 256 : n * 256 + 256].reshape(256, 256))
                z = z.astype(BF).reshape(16, 16, 256)
                if k == 0:
                    yrlat[0, :, half, n * 256 : n * 256 + 256] = z
                else:
                    yslat[k - 1, :, half, n * 256 : n * 256 + 256] = z

    def y_to(k):
        return (g, lax.rem(t + k, TP))

    def y_back(k):
        return (g, lax.rem(t + TP - k, TP))

    def y_copy(k, par, c):
        at = (pl.ds(c * 4, 4), pl.ds(par * 16, 16))
        n = (k - 1) * 8 + par * 4 + c
        return pltpu.make_async_remote_copy(
            src_ref=yslat.at[k - 1, at[0], at[1]],
            dst_ref=yrlat.at[k, at[0], at[1]],
            send_sem=yss.at[n], recv_sem=yrs.at[n], device_id=y_to(k), device_id_type=MESH,
        )

    def y_rope_copy(k, c):
        at, n = pl.ds(c * 4, 4), (k - 1) * 4 + c
        return pltpu.make_async_remote_copy(
            src_ref=ysrope.at[k - 1, at], dst_ref=yrrope.at[k, at],
            send_sem=yrss.at[n], recv_sem=yrrs.at[n], device_id=y_to(k), device_id_type=MESH,
        )

    def x_send(src, dst, ss, rs):
        for k in range(1, GROUPS):
            d = lax.rem(g + k, GROUPS)
            pltpu.make_async_remote_copy(
                src_ref=src.at[d], dst_ref=dst.at[g],
                send_sem=ss, recv_sem=rs, device_id=(d, t), device_id_type=MESH,
            ).start()
        dst[g] = src[g]

    def x_all(src, dst, ss, rs):
        many = pl.ds(0, GROUPS - 1)
        return pltpu.make_async_remote_copy(
            src_ref=src.at[many], dst_ref=dst.at[many],
            send_sem=ss, recv_sem=rs, device_id=(lax.rem(g + 1, GROUPS), t), device_id_type=MESH,
        )

    def forward(i):
        return xs.at[i], xr.at[i], xss.at[i], xrs.at[i]

    back_first = (bs, br, zss.at[0], zrs.at[0])
    back_second = (bs_c, br_c, zss.at[1], zrs.at[1])
    back_a = (bs_a, br_a, zss.at[3], zrs.at[3])
    back_b = (bs_b, br_b, zss.at[4], zrs.at[4])

    def place(i):
        for src, wide, at in ((qn_v, 256, 0), (qr_v, 128, 256)):
            rhs = jnp.concatenate(
                [src[:, (c * 4 + i) * wide : (c * 4 + i) * wide + wide] for c in range(4)], axis=0
            )
            for b in range(2):
                got = dot(sel_v[b * 256 : b * 256 + 256], rhs).astype(BF)
                xs[i, b * 16 : b * 16 + 16, :, at : at + wide] = got.reshape(16, 16, wide)

    with jax.named_scope("route"):
        sq = (128, 128)
        first = iota(sq, 0)
        lane1 = iota((1, 128), 1) & 63
        slot = jnp.zeros((1, 128), I32)
        for j in range(REQS):
            slot = jnp.where(lane1 == j, ps[rp[lax.rem(t * OWN + j, REQS)]], slot)
        slot = slot.astype(F32)
        slot_b = jnp.broadcast_to(slot, sq)
        before = first < (iota(sq, 1) & 63)
        rank = jnp.sum(jnp.where(before & (slot_b.T == slot_b), 1.0, 0.0), axis=0, keepdims=True)
        buf = jnp.broadcast_to(2.0 * slot + rank, sq)
        buf_r = buf.astype(I32)
        buf_c = buf.T.astype(I32)
        for b in range(4):
            i, j = iota(sq, 0) + b * 128, iota(sq, 1)
            key, col = (i >> 4) * 4 + (i & 3), (i >> 2) & 3
            for e in range(2):
                sel_v[b * 128 : b * 128 + 128, e * 128 : e * 128 + 128] = onehot(
                    (key == buf_r) & (col == ((j + e * 128) >> 6))
                )
    with jax.named_scope("masks"):
        for b in range(4):
            i, j = iota((128, 512), 0) + b * 128, iota((128, 512), 1)
            rows = pl.ds(b * 128, 128)
            slots_v[rows] = onehot(j == ((i >> 1) & 31) * 16 + (i >> 7) * 4 + ((i >> 6) & 1) * 2 + (i & 1))
            slotst_v[rows] = onehot(
                j == ((i >> 2) & 3) * 128 + ((i >> 1) & 1) * 64 + (i >> 4) * 2 + (i & 1)
            )
            i, j = iota(sq, 0), iota(sq, 1) + b * 128
            key, col = (j >> 4) * 4 + (j & 3), (j >> 2) & 3
            for e in range(2):
                selt_v[e * 128 : e * 128 + 128, b * 128 : b * 128 + 128] = onehot(
                    (key == buf_c) & (col == ((i + e * 128) >> 6))
                )
        i, j = iota((256, 256), 0), iota((256, 256), 1)
        permb_v[...] = onehot(j == (i & 7) * 32 + ((i >> 3) & 1) * 16 + (i >> 4))
    with jax.named_scope("wait_q"):
        pltpu.make_async_copy(qn, qn_v, lsem.at[0]).wait()
        pltpu.make_async_copy(qr, qr_v, lsem.at[1]).wait()
    with jax.named_scope("ropes"):
        for k in range(TP):
            rope = jnp.concatenate(
                [qr_v[k * OWN : k * OWN + OWN, hp * 128 : hp * 128 + 128] for hp in range(16)], axis=0
            )
            z = dot(perm_v[...], rope).astype(BF).reshape(16, 16, 128)
            if k == 0:
                yrrope[0] = z
            else:
                ysrope[k - 1] = z
    with jax.named_scope("place0"):
        place(0)
    with jax.named_scope("barrier"):
        pl.semaphore_wait(bar, TP - 1 + GROUPS - 1)
    for c in range(4):
        for k in range(1, TP):
            y_rope_copy(k, c).start()
    x_send(*forward(0))
    ld_wuk[0].wait()
    with jax.named_scope("qlat0"):
        q_latents(0)
    for k in range(1, TP):
        y_copy(k, 0, 0).start()
    with jax.named_scope("place"):
        for i in range(1, QUARTERS):
            place(i)
    for c in (ld_wuk[1], *ld_p):
        c.wait()
    with jax.named_scope("qlat1"):
        q_latents(1)
    for c in range(4):
        for par in range(2):
            for k in range(1, TP):
                if c or par:
                    y_copy(k, par, c).start()

    x_send(*forward(1))
    pst[...] = jnp.zeros_like(pst)
    stat_v[...] = jnp.zeros_like(stat_v)
    lane64 = iota((64, 128), 1)
    with jax.named_scope("loads"):
        ld_wuv.wait()
        for c in ld_s:
            c.wait()

    def scores(b, n):
        at = pl.ds(n * 256, 256)
        sc[b % 2, :, at] = dot(qb[b], kt_v[b % 2, :, at])

    def weigh(b, n):
        rows = slice(n * 32, n * 32 + 32)
        s = sc.at[b % 2]
        top = s[rows, 0:128]
        for m in range(1, PLEN // 128):
            top = jnp.maximum(top, s[rows, m * 128 : m * 128 + 128])
        top = jnp.max(top, axis=1, keepdims=True)
        top_b = jnp.broadcast_to(top * SCALE2, (32, 128))
        total = jnp.zeros((32, 128), F32)
        for m in range(PLEN // 256):
            e = [
                jnp.exp2(s[rows, at : at + 128] * SCALE2 - top_b)
                for at in (m * 256, m * 256 + 128)
            ]
            total = total + e[0] + e[1]
            pb[b % 2, rows, m * 256 : m * 256 + 256] = jnp.concatenate(e, axis=1).astype(BF)
        return top, jnp.sum(total, axis=1, keepdims=True)

    def values(b, n, inv):
        at = pl.ds(n * 256, 256)
        ob[b % 2, :, at] = (dot(pb[b % 2], pl_v[b % 2, :, at]) * inv).astype(BF)

    def give_back(rows, to, wide):
        for b in range(2):
            z = dot(slotst_v[b * 256 : b * 256 + 256], rows)
            to[b * 16 : b * 16 + 16] = z.astype(BF).reshape(16, 16, wide)

    def quarter(i, final=False):
        with jax.named_scope("wait_x"):
            x_all(*forward(i)).wait_recv()
        if not isinstance(i, int):
            x_send(*forward(i + 2))
        for b in range(2):
            for at, wide in ((0, 256), (256, 128)):
                cut = xr[i, :, :, at : at + wide].reshape(512, wide)
                rows = slice(b * 256, b * 256 + 256)
                qp[rows, at : at + wide] = dot(slots_v[rows], cut).astype(BF)
        lane = iota((128, 128), 1)
        for par in range(2):
            for c in range(4):
                rows = slice(c * 128, c * 128 + 128)
                y = dot(qp[rows, par * 128 : par * 128 + 128], wuk_v[c * 4 + i, par]).astype(BF)
                r = qp[rows, 256:384]
                r = jnp.where((lane < 64) if par == 0 else (lane >= 64), r, jnp.zeros_like(r))
                for p in range(2):
                    qb[par * 2 + p, c * 64 : c * 64 + 64, 0:LATENT] = y[p * 64 : p * 64 + 64]
                    qb[par * 2 + p, c * 64 : c * 64 + 64, LATENT : LATENT + 128] = r[p * 64 : p * 64 + 64]
        inv = {}
        for step in range(6):
            a, b, c = step, step - 1, step - 2
            parts = []
            for n in range(8):
                if a < 4:
                    scores(a, n)
                if 0 <= b < 4:
                    parts.append(weigh(b, n))
                if 0 <= c and n % 4 == 0:
                    values(c, n // 4, inv[c])
            if 0 <= b < 4:
                top = jnp.concatenate([x[0] for x in parts], axis=0)
                total = jnp.concatenate([x[1] for x in parts], axis=0)
                inv[b] = 1.0 / total
                lse = top * SCALE + jnp.log(total)
                hi = lse.astype(BF).astype(F32)
                mid = (lse - hi).astype(BF).astype(F32)
                lo = lse - hi - mid
                for e in range(4):
                    at = slice(e * 128 + (b % 2) * 64, e * 128 + (b % 2) * 64 + 64)
                    row = pst[at]
                    for n, part in enumerate((hi, mid, lo)):
                        at_lane = n * 32 + (b // 2) * 16 + e * 4 + i
                        row = jnp.where(lane64 == at_lane, part[e * 64 : e * 64 + 64], row)
                    pst[at] = row
            if c in (1, 3):
                par = c // 2
                for e in range(4):
                    rows = slice(e * 64, e * 64 + 64)
                    lhs = jnp.concatenate([ob[0, rows], ob[1, rows]], axis=0)
                    v = dot(lhs, wuv_v[e * 8 + 2 * i + par])
                    vq[e * 128 : e * 128 + 128, par * 128 : par * 128 + 128] = v.astype(BF)
                if final and par == 0:
                    give_back(vq[:, 0:128], bs_a, 128)
                    x_send(*back_a)
        if final:
            give_back(jnp.concatenate([vq[:, 128:256], pst[...].astype(BF)], axis=1), bs_b, 256)
            x_send(*back_b)
        elif isinstance(i, int):
            give_back(vq[...], bs_c, 256)
            x_send(*back_second)
        else:
            for b in range(2):
                z = dot(slotst_v[b * 256 : b * 256 + 256], vq[...])
                at = pl.ds(pl.multiple_of(i * 256, 256), 256)
                bs[b * 16 : b * 16 + 16, :, at] = z.astype(BF).reshape(16, 16, 256)

    srow, slane = iota((128, 128), 0), iota((128, 128), 1)

    def suffix(c):
        with jax.named_scope("wait_y"):
            for par in range(2):
                for k in range(1, TP):
                    y_copy(k, par, c).wait_recv()
            for k in range(1, TP):
                y_rope_copy(k, c).wait_recv()
        lane = iota((16, 128), 1)
        spos = iota((128, SLEN), 1)

        def match(j):
            r = c * 4 + j
            ql = jnp.concatenate([yrlat[k, r] for k in range(TP)], axis=0)
            parts = []
            for k in range(TP):
                x = yrrope[k, r]
                zero = jnp.zeros_like(x)
                parts += [jnp.where(lane < 64, x, zero), jnp.where(lane >= 64, x, zero)]
            s = lax.dot_general(ql, sl_v[r], (((1,), (1,)), ((), ())), preferred_element_type=F32)
            ss[j] = s + dot(jnp.concatenate(parts, axis=0), skr_v[r])

        def soft(j):
            r = c * 4 + j
            live = spos < slen[0, t * OWN + r]
            s = jnp.where(live, ss[j], -1e30)
            top = jnp.max(s, axis=1, keepdims=True)
            e = jnp.where(live, jnp.exp2((s - top) * SCALE2), 0.0)
            total = jnp.sum(e, axis=1, keepdims=True)
            es[j] = e.astype(BF)
            lse = top * SCALE + jnp.log(total)
            stat_v[...] = jnp.where(slane == (srow >> 5) * OWN + r, lse, stat_v[...])
            return 1.0 / total

        def mixed(j, inv):
            r = c * 4 + j
            for n in range(2):
                at = pl.ds(n * 256, 256)
                o = (dot(es[j], sl_v[r, :, at]) * inv).astype(BF)
                for k in range(TP):
                    o_v[k, r, :, at] = o[k * 32 : k * 32 + 32]

        inv = {}
        for step in range(6):
            if step < 4:
                match(step)
            if 0 <= step - 1 < 4:
                inv[step - 1] = soft(step - 1)
            if 0 <= step - 2:
                mixed(step - 2, inv[step - 2])

    def yb_copy(k, rh, q):
        at = pl.ds(q * 4, 4)
        n = (k - 1) * 8 + rh * 4 + q
        return pltpu.make_async_remote_copy(
            src_ref=ybs.at[k - 1, rh, at], dst_ref=ybr.at[k, rh, at],
            send_sem=bss.at[n], recv_sem=brs.at[n], device_id=y_back(k), device_id_type=MESH,
        )

    def yb_stat_copy(k):
        return pltpu.make_async_remote_copy(
            src_ref=ybs_st.at[k - 1], dst_ref=ybr_st.at[k],
            send_sem=bsts.at[k - 1], recv_sem=brts.at[k - 1], device_id=y_back(k), device_id_type=MESH,
        )

    def return_half(rh):
        for k in (1, 2, 3, 0):
            for n in range(2):
                cut = o_v[k, pl.ds(rh * 8, 8), :, n * 256 : n * 256 + 256].reshape(256, 256)
                z = dot(permb_v[...], cut).astype(BF).reshape(16, 16, 256)
                if k == 0:
                    ybr[0, rh, :, :, n * 256 : n * 256 + 256] = z
                else:
                    ybs[k - 1, rh, :, :, n * 256 : n * 256 + 256] = z
            if k == 3:
                for q in range(4):
                    for m in range(1, TP):
                        yb_copy(m, rh, q).start()

    def attend(j, carry):
        with jax.named_scope("quarter"):
            quarter(j)
        with jax.named_scope("suffix"):
            suffix(j)
        return carry

    def attend_suffix(j, carry):
        with jax.named_scope("suffix"):
            suffix(j)
        return carry

    lax.fori_loop(0, 2, attend, 0)
    with jax.named_scope("yback"):
        return_half(0)
    x_send(*back_first)
    with jax.named_scope("quarter"):
        quarter(2)
    lax.fori_loop(2, 4, attend_suffix, 0)
    for k in range(TP):
        part = stat_v[k * 32 : k * 32 + 32]
        if k == 0:
            ybr_st[0] = part
        else:
            ybs_st[k - 1] = part
    stats = [yb_stat_copy(k) for k in range(1, TP)]
    for c in stats:
        c.start()
    with jax.named_scope("yback"):
        return_half(1)
    with jax.named_scope("quarter"):
        quarter(3, True)

    def prefix_part(i):
        if i == 2:
            x_all(*back_second).wait_recv()
            back = br_c[...]
        else:
            if i == 0:
                x_all(*back_first).wait_recv()
            back = br[:, :, i * 256 : i * 256 + 256]
        pv_v[i] = dot(selt_v[...], back.reshape(512, 256))

    def suffix_part(q):
        with jax.named_scope("wait_yback"):
            for rh in range(2):
                for k in range(1, TP):
                    yb_copy(k, rh, q).wait_recv()
        for hp in range(q * 4, q * 4 + 4):
            lhs = jnp.concatenate([ybr[k, rh, hp] for k in range(TP) for rh in range(2)], axis=0)
            rhs = jnp.concatenate([wuv_v[2 * hp], wuv_v[2 * hp + 1]], axis=1)
            sv = dot(lhs, rhs)
            for par in range(2):
                h = 2 * hp + par
                sv_v[:, h * 128 : h * 128 + 128] = jnp.concatenate(
                    [sv[e * 16 + par * 8 : e * 16 + par * 8 + 8, par * 128 : par * 128 + 128] for e in range(8)],
                    axis=0,
                ).astype(BF)

    with jax.named_scope("parts"):
        for i in range(QUARTERS - 1):
            prefix_part(i)
        for i in range(QUARTERS - 1):
            suffix_part(i)
    with jax.named_scope("wait_stats"):
        for c in stats:
            c.wait_recv()
    st = ybr_st[0] + ybr_st[1] + ybr_st[2] + ybr_st[3]
    ls = jnp.concatenate([st, jnp.zeros((96, 128), F32)], axis=0).T[0:64]
    with jax.named_scope("wait_last"):
        x_all(*back_a).wait_recv()
        x_all(*back_b).wait_recv()
    pv_v[3, :, 0:128] = dot(selt_v[...], br_a[...].reshape(512, 128))
    last = dot(selt_v[...], br_b[...].reshape(512, 256))
    pv_v[3, :, 128:256] = last[:, 0:128]
    lp = jnp.zeros((64, 128), F32)
    for c in range(4):
        lp = lp + last[c * 64 : c * 64 + 64, 128:256]
    lp = lp + pltpu.roll(lp, 96, 1) + pltpu.roll(lp, 64, 1)
    top = jnp.maximum(lp, ls)
    a, b = jnp.exp(lp - top), jnp.exp(ls - top)
    inv = 1.0 / (a + b)
    a, b = a * inv, b * inv
    outs = []

    def finish(q):
        for h in range(q * 8, q * 8 + 8):
            i, par = h % 8 // 2, h % 2
            at, col = slice(h * 128, h * 128 + 128), par * 16 + h // 2
            prefix = pv_v[i, q * 64 : q * 64 + 64, par * 128 : par * 128 + 128]
            own = sv_v[:, at].astype(F32)
            out_v[:, at] = (a[:, col : col + 1] * prefix + b[:, col : col + 1] * own).astype(BF)
        for k in range(TP):
            c = pltpu.make_async_copy(
                out_v.at[pl.ds(k * OWN, OWN), pl.ds(q * 1024, 1024)],
                out.at[pl.ds(rel(k), OWN), pl.ds(q * 1024, 1024)],
                osem.at[q * 4 + k],
            )
            c.start()
            outs.append(c)

    with jax.named_scope("finish"):
        for q in range(3):
            finish(q)
    with jax.named_scope("last"):
        suffix_part(3)
        finish(3)
    with jax.named_scope("wait_sends"):
        for k in range(1, TP):
            for c in range(4):
                for par in range(2):
                    y_copy(k, par, c).wait_send()
                    yb_copy(k, par, c).wait_send()
        for k in range(1, TP):
            for c in range(4):
                y_rope_copy(k, c).wait_send()
        for c in stats:
            c.wait_send()
        for i in range(QUARTERS):
            x_all(*forward(i)).wait_send()
        x_all(*back_first).wait_send()
        x_all(*back_second).wait_send()
        x_all(*back_a).wait_send()
        x_all(*back_b).wait_send()
    with jax.named_scope("wait_out"):
        for c in outs:
            c.wait()


def local(qn, qr, wuk, wuv, plat, prope, slat, srope, slen, named, slot):
    hbm = pl.BlockSpec(memory_space=pl.ANY)
    smem = pl.BlockSpec(memory_space=pltpu.SMEM)

    def b(*shape):
        return pltpu.VMEM(shape, BF)

    def f(*shape):
        return pltpu.VMEM(shape, F32)

    def sem(n):
        return pltpu.SemaphoreType.DMA((n,))

    return pl.pallas_call(
        kernel,
        out_shape=jax.ShapeDtypeStruct((REQS, HEADS * VALUE), BF),
        in_specs=[hbm] * 8 + [smem] * 3,
        out_specs=hbm,
        scratch_shapes=[
            b(64, 4096), b(64, 2048), b(16, 2, 128, 512), b(32, 512, 128), b(2, 2048, 512), b(2, 640, 2048),
            b(16, 256, 512), b(16, 128, 256),
            b(512, 256), b(256, 512), b(256, 256), b(256, 256), b(512, 512), b(512, 512),
            b(4, 16, 16, 512), b(3, 16, 32, 512), b(4, 16, 32, 512), b(3, 16, 16, 128), b(4, 16, 16, 128),
            b(4, 16, 32, 512), b(3, 2, 16, 16, 512), b(4, 2, 16, 16, 512),
            f(128, 128), f(3, 32, 128), f(4, 32, 128),
            b(4, 32, 16, 384), b(4, 32, 16, 384), b(512, 384), b(512, 256), f(512, 128),
            b(32, 16, 512), b(32, 16, 512), b(32, 16, 256), b(32, 16, 256), b(32, 16, 128), b(32, 16, 128), b(32, 16, 256), b(32, 16, 256),
            b(4, 256, 640), f(2, 256, 2048), b(2, 256, 2048), b(2, 256, 512),
            f(4, 128, 256), b(4, 128, 256), f(4, 256, 256), b(64, 4096), b(64, 4096),
            sem(14), sem(16), sem(24), sem(24), sem(12), sem(12), sem(24), sem(24), sem(3), sem(3),
            sem(4), sem(4), sem(5), sem(5),
        ],
        compiler_params=pltpu.CompilerParams(
            collective_id=0, has_side_effects=True, vmem_limit_bytes=67043328
        ),
        name="attend",
    )(qn, qr, wuk.reshape(16, 2, NOPE, LATENT), wuv, plat, prope, slat, srope, named, slot, slen)


def solution(mesh):
    in_specs = (
        P("grp", "tp"), P("grp", "tp"), P("tp", None, None), P("tp", None, None),
        P("grp", None, None), P("grp", None, None), P(("grp", "tp"), None, None), P(("grp", "tp"), None, None),
        P("grp", None), P("grp"), P(),
    )
    return jax.shard_map(local, mesh=mesh, in_specs=in_specs, out_specs=P("grp", "tp"), check_vma=False)
```
